32 devices in a mesh: dp: 4 (over z), tp: 8 (over y, x, core).
Axes of the slice: x: 2, y: 2, z: 4, core: 2. Of those that a mesh axis runs over, the one named last changes fastest.
Arguments:
- x: bfloat16 [8, 1024, 4096], P('dp'), parts along dimension 0
- positions: int32 [8, 1024], P('dp'), parts along dimension 0
- lengths: int32 [8], P('dp'), parts along dimension 0
- w_q: bfloat16 [2, 4096, 4096], P(None, None, 'tp')
- w_k: bfloat16 [2, 4096, 1024], P(None, None, 'tp')
- w_v: bfloat16 [2, 4096, 1024], P(None, None, 'tp')
- w_o: bfloat16 [2, 4096, 4096], P(None, 'tp')
- w_gate: bfloat16 [2, 4096, 14336], P(None, None, 'tp')
- w_up: bfloat16 [2, 4096, 14336], P(None, None, 'tp')
- w_down: bfloat16 [2, 14336, 4096], P(None, 'tp')
- norm_gain: float32 [2, 4096], replicated
- q_gain: float32 [2, 32, 128], P(None, 'tp')
- k_gain: float32 [2, 8, 128], P(None, 'tp')
Outputs:
- output 1: bfloat16 [8, 1024, 4096], P('dp'), parts along dimension 0
- output 2: bfloat16 [2, 8, 1024, 8, 128], P(None, 'dp', None, 'tp'), parts along dimension 1
- output 3: bfloat16 [2, 8, 1024, 8, 128], P(None, 'dp', None, 'tp'), parts along dimension 1
There are 4 independent parts. The reference program is written for one: setup_inputs(seed, part) draws one part's arguments, and reference() takes and returns one part's arrays. A program takes and returns all parts, laid end to end along the dimension named above; an argument that names none is the same for every part.
All inputs are finite; a program needn't handle non-finite values.
Results may differ from the reference program's by a relative error of at most 0.0162269.
Values are sent between devices in bfloat16 or wider.
A program may use at most 1 GiB of HBM per device.

```python
import jax
import jax.numpy as jnp
from jax import lax

BATCH_ROWS = 2
SEQ_LEN = 1024
D_MODEL = 4096
N_HEADS = 32
KV_HEADS = 8
KV_SLOTS = 8
FF_WIDTH = 14336
N_LAYERS = 2
HEAD_DIM = 128
POS_OFFSET_RANGE = 8192
ROPE_THETA = 75000000.0
NORM_EPS = 1e-5


def setup_inputs(seed: int = 0, part: int = 0) -> dict:
    part_keys = jax.random.split(jax.random.fold_in(jax.random.key(seed), part), 4)
    shared_keys = jax.random.split(jax.random.key(seed + 1), 10)
    slot_copies = KV_SLOTS // KV_HEADS
    q_width = N_HEADS * HEAD_DIM

    def normal_weight(rng_key, arr_shape, fan_in, factor):
        return (jax.random.normal(rng_key, arr_shape, jnp.float32) * (factor * fan_in ** -0.5)).astype(jnp.bfloat16)

    def slot_weight(rng_key):
        head_draw = jax.random.normal(rng_key, (N_LAYERS, D_MODEL, KV_HEADS, HEAD_DIM), jnp.float32) * D_MODEL ** -0.5
        return jnp.repeat(head_draw, slot_copies, axis=2).reshape(N_LAYERS, D_MODEL, KV_SLOTS * HEAD_DIM).astype(jnp.bfloat16)

    def gain_draw(rng_key, arr_shape):
        return 1.0 + 0.3 * jax.random.normal(rng_key, arr_shape, jnp.float32)

    x = jax.random.normal(part_keys[0], (BATCH_ROWS, SEQ_LEN, D_MODEL), jnp.float32).astype(jnp.bfloat16)
    offsets = jax.random.randint(part_keys[1], (BATCH_ROWS,), 0, POS_OFFSET_RANGE, jnp.int32)
    positions = offsets[:, None] + jnp.arange(SEQ_LEN, dtype=jnp.int32)[None, :]
    drawn_lengths = jax.random.randint(part_keys[2], (BATCH_ROWS,), 1, SEQ_LEN + 1, jnp.int32)
    full_row = jax.random.randint(part_keys[3], (), 0, BATCH_ROWS, jnp.int32)
    lengths = jnp.where(jnp.arange(BATCH_ROWS, dtype=jnp.int32) == full_row, SEQ_LEN, drawn_lengths).astype(jnp.int32)
    out_factor = 2.0 * SEQ_LEN ** 0.125
    k_gain = jnp.repeat(gain_draw(shared_keys[9], (N_LAYERS, KV_HEADS, HEAD_DIM)), slot_copies, axis=1)
    return {
        'x': x,
        'positions': positions,
        'lengths': lengths,
        'w_q': normal_weight(shared_keys[0], (N_LAYERS, D_MODEL, q_width), D_MODEL, 1.0),
        'w_k': slot_weight(shared_keys[1]),
        'w_v': slot_weight(shared_keys[2]),
        'w_o': normal_weight(shared_keys[3], (N_LAYERS, q_width, D_MODEL), q_width, out_factor),
        'w_gate': normal_weight(shared_keys[4], (N_LAYERS, D_MODEL, FF_WIDTH), D_MODEL, 1.0),
        'w_up': normal_weight(shared_keys[5], (N_LAYERS, D_MODEL, FF_WIDTH), D_MODEL, 1.0),
        'w_down': normal_weight(shared_keys[6], (N_LAYERS, FF_WIDTH, D_MODEL), FF_WIDTH, 1.0),
        'norm_gain': gain_draw(shared_keys[7], (N_LAYERS, D_MODEL)),
        'q_gain': gain_draw(shared_keys[8], (N_LAYERS, N_HEADS, HEAD_DIM)),
        'k_gain': k_gain,
    }


def norm_rows(values, gain_vec):
    as_float = values.astype(jnp.float32)
    row_mean = jnp.mean(as_float, axis=-1, keepdims=True)
    centered = as_float - row_mean
    variance = jnp.mean(centered * centered, axis=-1, keepdims=True)
    return centered * lax.rsqrt(variance + NORM_EPS) * gain_vec


def apply_rope(values, cos_table, sin_table):
    pairs = values.reshape(values.shape[:-1] + (HEAD_DIM // 2, 2))
    even_part = pairs[..., 0]
    odd_part = pairs[..., 1]
    rotated = jnp.stack([even_part * cos_table - odd_part * sin_table, odd_part * cos_table + even_part * sin_table], axis=-1)
    return rotated.reshape(values.shape)


def reference(x, positions, lengths, w_q, w_k, w_v, w_o, w_gate, w_up, w_down, norm_gain, q_gain, k_gain):
    exponents = jnp.arange(HEAD_DIM // 2, dtype=jnp.float32) * (2.0 / HEAD_DIM)
    angles = positions.astype(jnp.float32)[:, :, None] * ROPE_THETA ** (-exponents)
    cos_table = jnp.cos(angles)[:, :, None, :]
    sin_table = jnp.sin(angles)[:, :, None, :]
    token_count = BATCH_ROWS * SEQ_LEN
    group_size = N_HEADS // KV_SLOTS
    seq_index = jnp.arange(SEQ_LEN)
    causal = seq_index[None, :] <= seq_index[:, None]
    score_scale = HEAD_DIM ** -0.5

    def attend_row(row_inputs):
        q_row, k_row, v_row, row_len = row_inputs
        allowed = causal & (seq_index[None, :] < row_len)
        q_first = jnp.transpose(q_row, (1, 0, 2))

        def one_head(head_idx):
            q_head = lax.dynamic_index_in_dim(q_first, head_idx, 0, keepdims=False)
            slot_idx = head_idx // group_size
            k_head = lax.dynamic_index_in_dim(k_row, slot_idx, 1, keepdims=False)
            v_head = lax.dynamic_index_in_dim(v_row, slot_idx, 1, keepdims=False)
            scores = jnp.dot(q_head, k_head.T, preferred_element_type=jnp.float32) * score_scale
            scores = jnp.where(allowed, scores, -1e30)
            attn_probs = jax.nn.softmax(scores, axis=-1).astype(jnp.bfloat16)
            return jnp.dot(attn_probs, v_head, preferred_element_type=jnp.float32).astype(jnp.bfloat16)

        head_outs = lax.map(one_head, jnp.arange(N_HEADS))
        return jnp.transpose(head_outs, (1, 0, 2)).reshape(SEQ_LEN, N_HEADS * HEAD_DIM)

    def layer_step(hidden, layer_weights):
        q_weight, k_weight, v_weight, o_weight, gate_weight, up_weight, down_weight, ln_gain, qn_gain, kn_gain = layer_weights
        normed = norm_rows(hidden, ln_gain).astype(jnp.bfloat16).reshape(token_count, D_MODEL)
        q_proj = jnp.dot(normed, q_weight, preferred_element_type=jnp.float32).reshape(BATCH_ROWS, SEQ_LEN, N_HEADS, HEAD_DIM)
        k_proj = jnp.dot(normed, k_weight, preferred_element_type=jnp.float32).reshape(BATCH_ROWS, SEQ_LEN, KV_SLOTS, HEAD_DIM)
        v_proj = jnp.dot(normed, v_weight, preferred_element_type=jnp.float32).astype(jnp.bfloat16).reshape(BATCH_ROWS, SEQ_LEN, KV_SLOTS, HEAD_DIM)
        q_rot = apply_rope(norm_rows(q_proj, qn_gain), cos_table, sin_table).astype(jnp.bfloat16)
        k_rot = apply_rope(norm_rows(k_proj, kn_gain), cos_table, sin_table).astype(jnp.bfloat16)
        attn_out = lax.map(attend_row, (q_rot, k_rot, v_proj, lengths)).reshape(token_count, N_HEADS * HEAD_DIM)
        gate_proj = jnp.dot(normed, gate_weight, preferred_element_type=jnp.float32)
        up_proj = jnp.dot(normed, up_weight, preferred_element_type=jnp.float32)
        mlp_act = (jax.nn.silu(gate_proj) * up_proj).astype(jnp.bfloat16)
        branch_sum = jnp.dot(attn_out, o_weight, preferred_element_type=jnp.float32) + jnp.dot(mlp_act, down_weight, preferred_element_type=jnp.float32)
        new_hidden = (hidden.reshape(token_count, D_MODEL).astype(jnp.float32) + branch_sum).astype(jnp.bfloat16)
        return new_hidden.reshape(BATCH_ROWS, SEQ_LEN, D_MODEL), (k_rot, v_proj)

    y, caches = lax.scan(layer_step, x, (w_q, w_k, w_v, w_o, w_gate, w_up, w_down, norm_gain, q_gain, k_gain))
    return y, caches[0], caches[1]
```

```python
import functools
import math

import jax
import jax.numpy as jnp
from jax import lax
from jax.experimental import pallas as pl
from jax.experimental.pallas import tpu as pltpu
from jax.sharding import PartitionSpec as P

HEAD = 128
ROPE_THETA = 75000000.0
NORM_EPS = 1e-5
BF = jnp.bfloat16
F32 = jnp.float32
MESH = pl.DeviceIdType.MESH
NG = 4
KINDS = 9
D2D, S1, S2, A2, A1A, A1B, A0A, A0B, A0C = range(KINDS)

LN_EV = {0: [("s0", 3)], 1: [("s1", 0)], 3: [("s1", 1)]}
ATT_EV = {0: [("s1", 2), ("s2", 0)], 1: [("s1", 3), ("s2", 1)]}
GU_EV = {0: [("a2", 0), ("s2", 2)], 1: [("a2", 1), ("s2", 3)], 2: [("a1", 0)], 3: [("a2", 2)], 4: [("a1", 1), ("a2", 3)], 5: [("a1", 2)], 6: [("a1", 3)]}
TAIL_EV = [("s0", 3), ("s1", 0), ("s1", 1), ("s2", 0), ("s1", 2), ("s2", 1), ("a2", 0), ("s1", 3), ("s2", 2), ("a2", 1), ("a1", 0), ("s2", 3), ("a2", 2), ("a1", 1), ("a2", 3), ("a1", 2), ("a1", 3)]


def mo(v, m):
    return pl.multiple_of(v, m)


def mega(cfg, lens, x, cos, sin, wq, wk, wv, wo, wg, wu, wd, ng, qg, kg,
         hy, kc, vc,
         wqkv, wgu, wdn, nbuf, hblk, ou, pbuf, d2d, s1b, s2b, res, qkvf, qbuf, kbuf, vbuf, csb,
         ssem, rsem, wsem, lsem, osem):
    CH, D, F, NH, NC, HS = cfg["CH"], cfg["D"], cfg["F"], cfg["NH"], cfg["NC"], cfg["HS"]
    GC = D // NG
    FT = cfg["FT"]
    NT = F // FT
    OW = NH * HEAD
    LB = CH // 4
    QB = CH // 4
    tp = lax.axis_index("tp")
    core = lax.rem(tp, 2)
    bx = lax.rem(lax.div(tp, 2), 2)
    by = lax.div(tp, 4)
    xn = tp + 2 - 4 * bx
    yn = tp + 4 - 8 * by
    cn = tp + 1 - 2 * core
    n1 = jnp.where(core == 0, xn, yn)
    n2 = jnp.where(core == 0, yn, xn)
    b1 = jnp.where(core == 0, bx, by)
    b2 = jnp.where(core == 0, by, bx)
    H2, H4, H8 = CH // 2, CH // 4, CH // 8
    my_row = core * H2 + b1 * H4 + b2 * H8

    def where(c):
        l = lax.div(c, 2 * HS)
        b = lax.rem(lax.div(c, HS), 2)
        s = lax.rem(c, HS)
        return l, b, s

    def rcopy(kind, c, g, src, dst, dev):
        par = lax.rem(c, 2)
        return pltpu.make_async_remote_copy(
            src_ref=src, dst_ref=dst, send_sem=ssem.at[kind, par, g], recv_sem=rsem.at[kind, par, g],
            device_id={"tp": dev}, device_id_type=MESH)

    def hrows(c, off, n, g):
        l, b, s = where(c)
        return hy.at[l, b, pl.ds(mo(s * CH + off, H8), n), pl.ds(mo(g * GC, GC), GC)]

    def k_d2d(c, g):
        par = lax.rem(c, 2)
        return rcopy(D2D, c, g, pbuf.at[g, pl.ds(mo((1 - core) * H2, H2), H2)], d2d.at[par, g], cn)

    def k_s1(c, g):
        par = lax.rem(c, 2)
        return rcopy(S1, c, g, d2d.at[par, g, pl.ds(mo((1 - b1) * H4, H4), H4)], s1b.at[par, g], n1)

    def k_s2(c, g):
        par = lax.rem(c, 2)
        return rcopy(S2, c, g, s1b.at[par, g, pl.ds(mo((1 - b2) * H8, H8), H8)], s2b.at[par, g], n2)

    def k_own(kind, c, g, dev):
        return rcopy(kind, c, g, s2b.at[lax.rem(c, 2), g], hrows(c, my_row, H8, g), dev)

    def k_fwd(kind, c, g, dev):
        if kind == A0C:
            off, n = core * H2 + (1 - b1) * H4, H4
        else:
            off, n = core * H2 + b1 * H4 + (1 - b2) * H8, H8
        ref = hrows(c, off, n, g)
        return rcopy(kind, c, g, ref, ref, dev)

    def k_loc(c, g):
        return pltpu.make_async_copy(s2b.at[lax.rem(c, 2), g], hrows(c, my_row, H8, g), lsem.at[2 + lax.rem(c, 2), g])

    def c_res(c):
        l, b, s = where(c)
        rows = pl.ds(mo(s * CH + my_row, H8), H8)
        return (pltpu.make_async_copy(x.at[b, rows], res, lsem.at[1, 0]),
                pltpu.make_async_copy(hy.at[0, b, rows], res, lsem.at[1, 0]))

    RB = min(32, H8)

    def s0(c, g):
        par = lax.rem(c, 2)
        cp = k_d2d(c, g)
        cp.wait_recv()
        cp.wait_send()

        @pl.loop(0, H2 // RB)
        def _(r):
            rr = pl.ds(mo(r * RB, RB), RB)
            d2d[par, g, rr] = d2d[par, g, rr] + pbuf[g, pl.ds(mo(core * H2 + r * RB, RB), RB)]
        k_s1(c, g).start()

    def s1(c, g):
        par = lax.rem(c, 2)
        cp = k_s1(c, g)
        cp.wait_recv()
        cp.wait_send()

        @pl.loop(0, H4 // RB)
        def _(r):
            rr = pl.ds(mo(r * RB, RB), RB)
            s1b[par, g, rr] = s1b[par, g, rr] + d2d[par, g, pl.ds(mo(b1 * H4 + r * RB, RB), RB)]
        k_s2(c, g).start()

    def s2(c, g):
        par = lax.rem(c, 2)
        cp = k_s2(c, g)
        cp.wait_recv()
        cp.wait_send()
        if g == 0:
            c_res(c)[0].wait()

        @pl.loop(0, H8 // RB)
        def _(r):
            rr = pl.ds(mo(r * RB, RB), RB)
            t = s2b[par, g, rr].astype(F32) + s1b[par, g, pl.ds(mo(b2 * H8 + r * RB, RB), RB)].astype(F32)
            s2b[par, g, rr] = (t + res[rr, pl.ds(g * GC, GC)].astype(F32)).astype(BF)
        k_own(A2, c, g, n2).start()
        k_own(A1A, c, g, n1).start()
        k_own(A0A, c, g, cn).start()
        k_loc(c, g).start()

    def a2(c, g):
        cp = k_own(A2, c, g, n2)
        cp.wait_recv()
        cp.wait_send()
        k_fwd(A1B, c, g, n1).start()
        k_fwd(A0B, c, g, cn).start()

    def a1(c, g):
        for cp in (k_own(A1A, c, g, n1), k_fwd(A1B, c, g, n1)):
            cp.wait_recv()
            cp.wait_send()
        k_fwd(A0C, c, g, cn).start()

    def a0(c):
        for g in range(NG):
            for cp in (k_own(A0A, c, g, cn), k_fwd(A0B, c, g, cn), k_fwd(A0C, c, g, cn)):
                cp.wait_recv()
                cp.wait_send()
            k_loc(c, g).wait()

    handlers = {"s0": s0, "s1": s1, "s2": s2, "a2": a2, "a1": a1}

    def events(c, evs, extra=None):
        if evs:
            @pl.when(c >= 0 if extra is None else (c >= 0) & extra)
            def _():
                for name, g in evs:
                    handlers[name](c, g)

    def c_qkv(l):
        return (pltpu.make_async_copy(wq.at[l], wqkv.at[:, pl.ds(0, OW)], wsem.at[0, 0]),
                pltpu.make_async_copy(wk.at[l], wqkv.at[:, pl.ds(OW, HEAD)], wsem.at[0, 1]),
                pltpu.make_async_copy(wv.at[l], wqkv.at[:, pl.ds(OW + HEAD, HEAD)], wsem.at[0, 2]))

    def c_gu(l, j):
        sl = lax.rem(j, 2)
        cc = pl.ds(mo(j * FT, FT), FT)
        return (pltpu.make_async_copy(wg.at[l, :, cc], wgu.at[sl, :, pl.ds(0, FT)], wsem.at[1, sl]),
                pltpu.make_async_copy(wu.at[l, :, cc], wgu.at[sl, :, pl.ds(FT, FT)], wsem.at[2, sl]))

    def c_dn(l, g):
        sl = lax.rem(g, 2)
        cc = pl.ds(mo(g * GC, GC), GC)
        return (pltpu.make_async_copy(wo.at[l, :, cc], wdn.at[sl, pl.ds(0, OW)], wsem.at[3, sl]),
                pltpu.make_async_copy(wd.at[l, :, cc], wdn.at[sl, pl.ds(OW, F)], wsem.at[4, sl]))

    def c_h(c, r):
        l, b, s = where(c)
        sl = lax.rem(r, 2)
        rows = pl.ds(mo(s * CH + r * LB, LB), LB)
        return (pltpu.make_async_copy(x.at[b, rows], hblk.at[sl], lsem.at[0, sl]),
                pltpu.make_async_copy(hy.at[0, b, rows], hblk.at[sl], lsem.at[0, sl]))

    def c_cs(c):
        l, b, s = where(c)
        rows = pl.ds(mo(s * CH, CH), CH)
        return (pltpu.make_async_copy(cos.at[b, rows], csb.at[0], wsem.at[5, 0]),
                pltpu.make_async_copy(sin.at[b, rows], csb.at[1], wsem.at[5, 1]))

    def c_kv(c):
        l, b, s = where(c)
        rows = pl.ds(mo(s * CH, CH), CH)
        return (pltpu.make_async_copy(kbuf.at[rows], kc.at[l, b, rows], osem.at[0]),
                pltpu.make_async_copy(vbuf.at[rows], vc.at[l, b, rows], osem.at[1]))

    def start(cps):
        for cp in cps:
            cp.start()

    def wait(cps):
        for cp in cps:
            cp.wait()

    def start_by_layer(c, pair):
        @pl.when(c < 2 * HS)
        def _():
            pair[0].start()

        @pl.when(c >= 2 * HS)
        def _():
            pair[1].start()

    bar = pltpu.get_barrier_semaphore()
    for dev in (xn, yn, cn):
        pl.semaphore_signal(bar, inc=1, device_id={"tp": dev}, device_id_type=MESH)

    start(c_qkv(0))
    c_h(0, 0)[0].start()
    start(c_cs(0))
    pl.semaphore_wait(bar, 3)

    @pl.loop(0, NC)
    def _(i):
        l, b, s = where(i)
        c = i - 1

        @pl.when(i >= 2)
        def _():
            a0(i - 2)

        gain = ng[pl.ds(l, 1), :]

        @pl.loop(0, CH // LB)
        def _(r):
            c_h(i, r)[0].wait()

            @pl.when(r + 1 < CH // LB)
            def _():
                start_by_layer(i, c_h(i, r + 1))
            for k, evs in LN_EV.items():
                events(c, evs, r == k)
            sl = lax.rem(r, 2)

            @pl.loop(0, LB // 16)
            def _(q):
                v = hblk[sl, pl.ds(mo(q * 16, 16), 16), :].astype(F32)
                mean = jnp.sum(v, axis=1, keepdims=True) * (1.0 / D)
                v = v - mean
                var = jnp.sum(v * v, axis=1, keepdims=True) * (1.0 / D)
                nbuf[pl.ds(mo(r * LB + q * 16, 16), 16), :] = (v * lax.rsqrt(var + NORM_EPS) * gain).astype(BF)

        wait(c_qkv(l))
        start(c_gu(l, 0))

        @pl.when(i > 0)
        def _():
            wait(c_kv(i - 1))
        qkvf[...] = jnp.dot(nbuf[...], wqkv[...], preferred_element_type=F32)
        wait(c_cs(i))
        lane = lax.broadcasted_iota(jnp.int32, (64, HEAD), 1)
        even = lax.rem(lane, 2) == 0

        @pl.loop(0, CH // 64)
        def _(r):
            rr = pl.ds(mo(r * 64, 64), 64)
            ct = csb[0, rr]
            st = csb[1, rr]

            def norm_rope(v, gvec):
                mean = jnp.sum(v, axis=1, keepdims=True) * (1.0 / HEAD)
                v = v - mean
                var = jnp.sum(v * v, axis=1, keepdims=True) * (1.0 / HEAD)
                v = v * lax.rsqrt(var + NORM_EPS) * gvec
                sw = jnp.where(even, pltpu.roll(v, HEAD - 1, 1), pltpu.roll(v, 1, 1))
                return (v * ct + sw * st).astype(BF)
            for h in range(NH):
                qbuf[h, rr] = norm_rope(qkvf[rr, pl.ds(h * HEAD, HEAD)], qg[l, pl.ds(h, 1), :])
            ks = pl.ds(mo(s * CH + r * 64, 64), 64)
            kbuf[ks] = norm_rope(qkvf[rr, pl.ds(OW, HEAD)], kg[l])
            vbuf[ks] = qkvf[rr, pl.ds(OW + HEAD, HEAD)].astype(BF)

        start(c_kv(i))

        @pl.when(i + 1 < NC)
        def _():
            start(c_cs(i + 1))
        rlen = lens[b]
        scale = HEAD ** -0.5

        def attn(s_static, qb):
            base = s_static * CH + qb * QB
            nk = base + QB
            q4 = qbuf[:, pl.ds(qb * QB, QB), :].reshape(NH * QB, HEAD)
            sc = lax.dot_general(q4, kbuf[pl.ds(0, nk)], (((1,), (1,)), ((), ())), preferred_element_type=F32)
            kid = lax.broadcasted_iota(jnp.int32, (QB, nk), 1)
            qid = lax.broadcasted_iota(jnp.int32, (QB, nk), 0) + base
            bias = jnp.where((kid <= qid) & (kid < rlen), 0.0, -1e30)
            sc = sc.reshape(NH, QB, nk) * scale + bias[None]
            m = jnp.max(sc, axis=2, keepdims=True)
            e = jnp.exp(sc - m)
            pr = (e * (1.0 / jnp.sum(e, axis=2, keepdims=True))).astype(BF)
            o = jnp.dot(pr.reshape(NH * QB, nk), vbuf[pl.ds(0, nk)], preferred_element_type=F32).astype(BF)
            for h in range(NH):
                ou[pl.ds(qb * QB, QB), pl.ds(h * HEAD, HEAD)] = o[h * QB:(h + 1) * QB]

        for half in range(2):
            events(c, ATT_EV.get(half))
            for ss in range(HS):
                @pl.when(s == ss)
                def _():
                    for qb in range(half * 2, half * 2 + 2):
                        attn(ss, qb)

        @pl.loop(0, NT)
        def _(j):
            wait(c_gu(l, j))

            @pl.when(j + 1 < NT)
            def _():
                start(c_gu(l, j + 1))

            @pl.when(j + 1 == NT)
            def _():
                start(c_dn(l, 0))
            for k, evs in GU_EV.items():
                events(c, evs, j == min(k, NT - 1))
            r = jnp.dot(nbuf[...], wgu[lax.rem(j, 2)], preferred_element_type=F32)
            ou[:, pl.ds(mo(OW + j * FT, 128), FT)] = (jax.nn.silu(r[:, :FT]) * r[:, FT:]).astype(BF)

        @pl.when(i + 1 < NC)
        def _():
            start(c_qkv(where(i + 1)[0]))
            start_by_layer(i + 1, c_h(i + 1, 0))
        start_by_layer(i, c_res(i))

        @pl.loop(0, NG)
        def _(g):
            wait(c_dn(l, g))

            @pl.when(g + 1 < NG)
            def _():
                start(c_dn(l, g + 1))

            @pl.when(g >= 2)
            def _():
                s0(i, g - 2)
            pbuf[g] = jnp.dot(ou[...], wdn[lax.rem(g, 2)], preferred_element_type=F32).astype(BF)
            k_d2d(i, g).start()
        s0(i, 2)

    a0(NC - 2)
    for name, g in TAIL_EV:
        handlers[name](NC - 1, g)
    a0(NC - 1)
    wait(c_kv(NC - 1))


def build(cfg, lens, x, cos, sin, wq, wk, wv, wo, wg, wu, wd, ng, qg, kg):
    CH, D, F, NH, HS = cfg["CH"], cfg["D"], cfg["F"], cfg["NH"], cfg["HS"]
    L, S = wq.shape[0], x.shape[1]
    OW = NH * HEAD
    GC = D // NG
    FT = cfg["FT"]
    any_ = pl.BlockSpec(memory_space=pltpu.HBM)
    vm = pl.BlockSpec(memory_space=pltpu.VMEM)
    V = pltpu.VMEM
    dma = pltpu.SemaphoreType.DMA
    T = 2 * S
    fl = L * (2 * T * D * (OW + 2 * HEAD + 2 * F) + 2 * T * (OW + F) * D)
    return pl.pallas_call(
        functools.partial(mega, cfg),
        name="mega",
        out_shape=(jax.ShapeDtypeStruct((L, 2, S, D), BF), jax.ShapeDtypeStruct((L, 2, S, HEAD), BF), jax.ShapeDtypeStruct((L, 2, S, HEAD), BF)),
        in_specs=[pl.BlockSpec(memory_space=pltpu.SMEM)] + [any_] * 10 + [vm] * 3,
        out_specs=(any_, any_, any_),
        scratch_shapes=[
            V((D, OW + 2 * HEAD), BF), V((2, D, 2 * FT), BF), V((2, OW + F, GC), BF),
            V((CH, D), BF), V((2, CH // 4, D), BF), V((CH, OW + F), BF),
            V((NG, CH, GC), BF), V((2, NG, CH // 2, GC), BF), V((2, NG, CH // 4, GC), BF), V((2, NG, CH // 8, GC), BF),
            V((CH // 8, D), BF), V((CH, OW + 2 * HEAD), F32), V((NH, CH, HEAD), BF), V((S, HEAD), BF), V((S, HEAD), BF),
            V((2, CH, HEAD), F32),
            dma((KINDS, 2, NG)), dma((KINDS, 2, NG)), dma((6, 3)), dma((4, NG)), dma((2,)),
        ],
        compiler_params=pltpu.CompilerParams(collective_id=0, has_side_effects=True, vmem_limit_bytes=66 * 10 ** 6),
        cost_estimate=pl.CostEstimate(flops=fl, bytes_accessed=200 * 2 ** 20, transcendentals=0),
    )(lens, x, cos, sin, wq, wk, wv, wo, wg, wu, wd, ng, qg, kg)


def rope_tables(positions):
    pair = jnp.arange(HEAD // 2, dtype=F32) * (2.0 / HEAD)
    freq = jnp.repeat(ROPE_THETA ** (-pair), 2)
    ang = positions.astype(F32)[:, :, None] * freq
    sign = jnp.where(jnp.arange(HEAD) % 2 == 0, -1.0, 1.0).astype(F32)
    return jnp.cos(ang), jnp.sin(ang) * sign


def solution(mesh, ch=512, ft=256):
    act = P("dp", None, None)
    col = P(None, None, "tp")
    row = P(None, "tp", None)
    cache = P(None, "dp", None, "tp", None)

    def body(x, positions, lengths, w_q, w_k, w_v, w_o, w_gate, w_up, w_down, norm_gain, q_gain, k_gain):
        L, S = w_q.shape[0], x.shape[1]
        hs = S // ch
        cfg = dict(CH=ch, D=x.shape[2], F=w_gate.shape[2], NH=q_gain.shape[1], NC=L * 2 * hs, HS=hs, FT=ft)
        cos, sin = rope_tables(positions)
        hy, kc, vc = build(cfg, lengths, x, cos, sin, w_q, w_k, w_v, w_o, w_gate, w_up, w_down, norm_gain, q_gain, k_gain)
        return hy[L - 1], kc[:, :, :, None, :], vc[:, :, :, None, :]

    return jax.shard_map(body, mesh=mesh, in_specs=(act, P("dp", None), P("dp"), col, col, col, row, col, col, row, P(None, None), row, row),
                         out_specs=(act, cache, cache), check_vma=False)
```

```python
import functools
import math

import jax
import jax.numpy as jnp
from jax import lax
from jax.experimental import pallas as pl
from jax.experimental.pallas import tpu as pltpu
from jax.sharding import PartitionSpec as P

HEAD = 128
ROPE_THETA = 75000000.0
NORM_EPS = 1e-5
BF = jnp.bfloat16
F32 = jnp.float32
MESH = pl.DeviceIdType.MESH
NG = 4
KINDS = 9
D2D, S1, S2, A2, A1A, A1B, A0A, A0B, A0C = range(KINDS)

Q_EV = [("a1", 2, 2)]
ROPE_EV = {0: [("s0", 1, 3), ("s1", 1, 0), ("a1", 2, 3)], 1: [("s1", 1, 1)]}
ATT_EV = [("s1", 1, 2)]
GU_EV = {2: [("s1", 1, 3), ("s2", 1, 0)], 3: [("s2", 1, 1)], 4: [("s2", 1, 2), ("a2", 1, 0), ("a0", 2, 0)], 5: [("s2", 1, 3)], 6: [("a2", 1, 1)]}
DN_EV = {0: [("a2", 1, 2)], 1: [("a2", 1, 3), ("a1", 1, 0)], 2: [("s0", 0, 0)], 3: [("s0", 0, 1), ("a1", 1, 1)]}
END_EV = [("s0", 0, 2)]
TAIL_EV = [("a1", 2, 2), ("a1", 2, 3), ("s0", 1, 3), ("s1", 1, 0), ("s1", 1, 1), ("s2", 1, 0), ("s1", 1, 2), ("s2", 1, 1), ("a2", 1, 0), ("s1", 1, 3), ("s2", 1, 2), ("a2", 1, 1), ("a1", 1, 0),
           ("s2", 1, 3), ("a2", 1, 2), ("a1", 1, 1), ("a2", 1, 3), ("a1", 1, 2), ("a1", 1, 3)]


def mo(v, m):
    return pl.multiple_of(v, m)


def mega(cfg, lens, x, cos, sin, wq, wk, wv, wo, wg, wu, wd, ng, qg, kg,
         hy, kc, vc,
         wqkv, ring, wdn, nbuf, hblk, ou, pbuf, d2d, s1b, s2b, res, qbuf, sbuf, prob, lbias, kbuf, vbuf, csb,
         ssem, rsem, wsem, lsem, osem):
    CH, D, F, NH, NC, HS = cfg["CH"], cfg["D"], cfg["F"], cfg["NH"], cfg["NC"], cfg["HS"]
    GC = D // NG
    FT = cfg["FT"]
    NT = F // FT
    OW = NH * HEAD
    S = HS * CH
    QB = CH // 4
    tp = lax.axis_index("tp")
    core = lax.rem(tp, 2)
    bx = lax.rem(lax.div(tp, 2), 2)
    by = lax.div(tp, 4)
    xn = tp + 2 - 4 * bx
    yn = tp + 4 - 8 * by
    cn = tp + 1 - 2 * core
    n1 = jnp.where(core == 0, xn, yn)
    n2 = jnp.where(core == 0, yn, xn)
    b1 = jnp.where(core == 0, bx, by)
    b2 = jnp.where(core == 0, by, bx)
    H2, H4, H8 = CH // 2, CH // 4, CH // 8
    my_row = core * H2 + b1 * H4 + b2 * H8

    def where(c):
        l = lax.div(c, 2 * HS)
        b = lax.rem(lax.div(c, HS), 2)
        s = lax.rem(c, HS)
        return l, b, s

    def rcopy(kind, c, g, src, dst, dev):
        par = lax.rem(c, 2)
        return pltpu.make_async_remote_copy(
            src_ref=src, dst_ref=dst, send_sem=ssem.at[kind, par, g], recv_sem=rsem.at[kind, par, g],
            device_id={"tp": dev}, device_id_type=MESH)

    def hrows(c, off, n, g):
        l, b, s = where(c)
        return hy.at[l, b, pl.ds(mo(s * CH + off, H8), n), pl.ds(mo(g * GC, GC), GC)]

    def k_d2d(c, g):
        par = lax.rem(c, 2)
        return rcopy(D2D, c, g, pbuf.at[g, pl.ds(mo((1 - core) * H2, H2), H2)], d2d.at[par, g], cn)

    def k_s1(c, g):
        par = lax.rem(c, 2)
        return rcopy(S1, c, g, d2d.at[par, g, pl.ds(mo((1 - b1) * H4, H4), H4)], s1b.at[par, g], n1)

    def k_s2(c, g):
        par = lax.rem(c, 2)
        return rcopy(S2, c, g, s1b.at[par, g, pl.ds(mo((1 - b2) * H8, H8), H8)], s2b.at[par, g], n2)

    def k_own(kind, c, g, dev):
        return rcopy(kind, c, g, s2b.at[lax.rem(c, 2), g], hrows(c, my_row, H8, g), dev)

    def k_fwd(kind, c, g, dev):
        if kind == A0C:
            off, n = core * H2 + (1 - b1) * H4, H4
        else:
            off, n = core * H2 + b1 * H4 + (1 - b2) * H8, H8
        ref = hrows(c, off, n, g)
        return rcopy(kind, c, g, ref, ref, dev)

    def k_loc(c, g):
        return pltpu.make_async_copy(s2b.at[lax.rem(c, 2), g], hrows(c, my_row, H8, g), lsem.at[2 + lax.rem(c, 2), g])

    def c_res(c):
        l, b, s = where(c)
        rows = pl.ds(mo(s * CH + my_row, H8), H8)
        return (pltpu.make_async_copy(x.at[b, rows], res, lsem.at[1, 0]),
                pltpu.make_async_copy(hy.at[0, b, rows], res, lsem.at[1, 0]))

    RB = min(32, H8)

    def s0(c, g):
        par = lax.rem(c, 2)
        cp = k_d2d(c, g)
        cp.wait_recv()
        cp.wait_send()

        @pl.loop(0, H2 // RB)
        def _(r):
            rr = pl.ds(mo(r * RB, RB), RB)
            d2d[par, g, rr] = d2d[par, g, rr] + pbuf[g, pl.ds(mo(core * H2 + r * RB, RB), RB)]
        k_s1(c, g).start()

    def s1(c, g):
        par = lax.rem(c, 2)
        cp = k_s1(c, g)
        cp.wait_recv()
        cp.wait_send()

        @pl.loop(0, H4 // RB)
        def _(r):
            rr = pl.ds(mo(r * RB, RB), RB)
            s1b[par, g, rr] = s1b[par, g, rr] + d2d[par, g, pl.ds(mo(b1 * H4 + r * RB, RB), RB)]
        k_s2(c, g).start()

    def s2(c, g):
        par = lax.rem(c, 2)
        cp = k_s2(c, g)
        cp.wait_recv()
        cp.wait_send()
        if g == 0:
            c_res(c)[0].wait()

        @pl.loop(0, H8 // RB)
        def _(r):
            rr = pl.ds(mo(r * RB, RB), RB)
            t = s2b[par, g, rr].astype(F32) + s1b[par, g, pl.ds(mo(b2 * H8 + r * RB, RB), RB)].astype(F32)
            s2b[par, g, rr] = (t + res[rr, pl.ds(g * GC, GC)].astype(F32)).astype(BF)
        k_own(A2, c, g, n2).start()
        k_own(A1A, c, g, n1).start()
        k_own(A0A, c, g, cn).start()
        k_loc(c, g).start()

    def a2(c, g):
        cp = k_own(A2, c, g, n2)
        cp.wait_recv()
        cp.wait_send()
        k_fwd(A1B, c, g, n1).start()
        k_fwd(A0B, c, g, cn).start()

    def a1(c, g):
        for cp in (k_own(A1A, c, g, n1), k_fwd(A1B, c, g, n1)):
            cp.wait_recv()
            cp.wait_send()
        k_fwd(A0C, c, g, cn).start()

    def a0(c, _):
        for g in range(NG):
            for cp in (k_own(A0A, c, g, cn), k_fwd(A0B, c, g, cn), k_fwd(A0C, c, g, cn)):
                cp.wait_recv()
                cp.wait_send()
            k_loc(c, g).wait()

    handlers = {"s0": s0, "s1": s1, "s2": s2, "a2": a2, "a1": a1, "a0": a0}

    def events(i, evs, extra=None):
        for lag in (2, 1, 0):
            now = [(name, g) for name, d, g in evs if d == lag]
            if not now:
                continue
            ok = i >= lag

            @pl.when(ok if extra is None else ok & extra)
            def _():
                for name, g in now:
                    handlers[name](i - lag, g)

    def c_qkv(l):
        return (pltpu.make_async_copy(wq.at[l], wqkv.at[:, pl.ds(0, OW)], wsem.at[5, 0]),
                pltpu.make_async_copy(wk.at[l], wqkv.at[:, pl.ds(OW, HEAD)], wsem.at[5, 1]),
                pltpu.make_async_copy(wv.at[l], wqkv.at[:, pl.ds(OW + HEAD, HEAD)], wsem.at[5, 2]))

    def c_gu(c, j):
        l = where(c)[0]
        sl = lax.rem(c * NT + j, 3)
        cc = pl.ds(mo(j * FT, FT), FT)
        return (pltpu.make_async_copy(wg.at[l, :, cc], ring.at[sl, :, pl.ds(0, FT)], wsem.at[0, sl]),
                pltpu.make_async_copy(wu.at[l, :, cc], ring.at[sl, :, pl.ds(FT, FT)], wsem.at[1, sl]))

    def c_dn(l, g):
        sl = lax.rem(g, 2)
        cc = pl.ds(mo(g * GC, GC), GC)
        return (pltpu.make_async_copy(wo.at[l, :, cc], wdn.at[sl, pl.ds(0, OW)], wsem.at[2, sl]),
                pltpu.make_async_copy(wd.at[l, :, cc], wdn.at[sl, pl.ds(OW, F)], wsem.at[3, sl]))

    UB, UN = CH // 8, 5
    US = (CH - UN * UB) // NG

    def c_h(c, off, n, sl):
        l, b, s = where(c)
        rows = pl.ds(mo(s * CH + off, 16), n)
        dst = hblk.at[sl, pl.ds(0, n)]
        return (pltpu.make_async_copy(x.at[b, rows], dst, lsem.at[0, sl]),
                pltpu.make_async_copy(hy.at[0, b, rows], dst, lsem.at[0, sl]))

    def c_hgu(c, u):
        return c_h(c, u * UB, UB, lax.rem(u, 2))

    def c_hdn(c, g):
        return c_h(c, UN * UB + g * US, US, lax.rem(UN + g, 2))

    def c_cs(c):
        l, b, s = where(c)
        rows = pl.ds(mo(s * CH, CH), CH)
        return (pltpu.make_async_copy(cos.at[b, rows], csb.at[0], wsem.at[4, 0]),
                pltpu.make_async_copy(sin.at[b, rows], csb.at[1], wsem.at[4, 1]))

    def c_kv(c):
        l, b, s = where(c)
        rows = pl.ds(mo(s * CH, CH), CH)
        return (pltpu.make_async_copy(kbuf.at[rows], kc.at[l, b, rows], osem.at[0]),
                pltpu.make_async_copy(vbuf.at[rows], vc.at[l, b, rows], osem.at[1]))

    def start(cps):
        for cp in cps:
            cp.start(priority=1)

    def wait(cps):
        for cp in cps:
            cp.wait()

    def start_by_layer(c, pair):
        @pl.when(c < 2 * HS)
        def _():
            pair[0].start()

        @pl.when(c >= 2 * HS)
        def _():
            pair[1].start()

    bar = pltpu.get_barrier_semaphore()
    for dev in (xn, yn, cn):
        pl.semaphore_signal(bar, inc=1, device_id={"tp": dev}, device_id_type=MESH)

    def ln_rows(src, dst, gain, n):
        for q in range(n // 16):
            v = src(q).astype(F32)
            mean = jnp.sum(v, axis=1, keepdims=True) * (1.0 / D)
            v = v - mean
            var = jnp.sum(v * v, axis=1, keepdims=True) * (1.0 / D)
            dst(q, (v * lax.rsqrt(var + NORM_EPS) * gain).astype(BF))

    def ln_first(src, dst, gain, n):
        means = [jnp.sum(src(q).astype(F32), axis=1, keepdims=True) * (1.0 / D) for q in range(n // 16)]
        rs = []
        for q in range(n // 16):
            v = src(q).astype(F32) - means[q]
            rs.append(lax.rsqrt(jnp.sum(v * v, axis=1, keepdims=True) * (1.0 / D) + NORM_EPS))
        for q in range(n // 16):
            dst(q, ((src(q).astype(F32) - means[q]) * rs[q] * gain).astype(BF))

    def ln_next(i, off, n, sl):
        par = lax.rem(i + 1, 2)
        gain = ng[pl.ds(jnp.minimum(lax.div(i + 1, 2 * HS), ng.shape[0] - 1), 1), :]

        def put(q, v):
            nbuf[par, pl.ds(mo(off + q * 16, 16), 16), :] = v
        ln_rows(lambda q: hblk[sl, pl.ds(q * 16, 16), :], put, gain, n)

    def first(k):
        rows = pl.ds(mo(k * UB, UB), UB)
        return pltpu.make_async_copy(x.at[0, rows], nbuf.at[1, rows], lsem.at[2 + lax.div(k, 4), lax.rem(k, 4)])

    for k in range(8):
        first(k).start()
    start(c_qkv(0))
    for cp in c_cs(0):
        cp.start()
    start(c_gu(0, 0))
    start(c_gu(0, 1))
    gain0 = ng[pl.ds(0, 1), :]

    @pl.loop(0, 8)
    def _(k):
        first(k).wait()

        def put(q, v):
            nbuf[0, pl.ds(mo(k * UB + q * 16, 16), 16), :] = v
        ln_first(lambda q: nbuf[1, pl.ds(mo(k * UB + q * 16, 16), 16), :], put, gain0, UB)

    pl.semaphore_wait(bar, 3)
    lane = lax.broadcasted_iota(jnp.int32, (CH // 2, HEAD), 1)
    even = lax.rem(lane, 2) == 0

    @pl.loop(0, NC)
    def _(i):
        l, b, s = where(i)
        np_ = lax.rem(i, 2)
        more = i + 1 < NC
        lnext = where(i + 1)[0]

        wait(c_qkv(l))
        events(i, Q_EV)

        @pl.when(i > 0)
        def _():
            wait(c_kv(i - 1))
        wait(c_cs(i))
        sbuf[1, :, pl.ds(0, OW + 2 * HEAD)] = jnp.dot(nbuf[np_], wqkv[...], preferred_element_type=F32)

        def gu(j):
            r = jnp.dot(nbuf[np_], ring[lax.rem(i * NT + j, 3)], preferred_element_type=F32)
            ou[:, pl.ds(mo(OW + j * FT, 128), FT)] = (jax.nn.silu(r[:, :FT]) * r[:, FT:]).astype(BF)

        @pl.loop(0, 2)
        def _(j):
            wait(c_gu(i, j))
            start(c_gu(i, j + 2))
            for k, evs in ROPE_EV.items():
                events(i, evs, j == k)
            rr = pl.ds(mo(j * H2, H2), H2)
            ct = csb[0, rr]
            st = csb[1, rr]

            def norm_rope(v, gvec):
                mean = jnp.sum(v, axis=1, keepdims=True) * (1.0 / HEAD)
                v = v - mean
                var = jnp.sum(v * v, axis=1, keepdims=True) * (1.0 / HEAD)
                v = v * lax.rsqrt(var + NORM_EPS) * gvec
                sw = jnp.where(even, pltpu.roll(v, HEAD - 1, 1), pltpu.roll(v, 1, 1))
                return (v * ct + sw * st).astype(BF)
            for h in range(NH):
                qbuf[h, rr] = norm_rope(sbuf[1, rr, pl.ds(h * HEAD, HEAD)], qg[l, pl.ds(h, 1), :])
            ks = pl.ds(mo(s * CH + j * H2, H2), H2)
            kbuf[ks] = norm_rope(sbuf[1, rr, pl.ds(OW, HEAD)], kg[l])
            vbuf[ks] = sbuf[1, rr, pl.ds(OW + HEAD, HEAD)].astype(BF)
            gu(j)

        for cp in c_kv(i):
            cp.start()

        @pl.when(more)
        def _():
            for cp in c_cs(i + 1):
                cp.start()
            start_by_layer(i + 1, c_hgu(i + 1, 0))
        events(i, ATT_EV)
        rlen = lens[b]
        sscale = HEAD ** -0.5 * math.log2(math.e)

        def qk(ss, qb):
            q4 = qbuf[:, pl.ds(qb * QB, QB), :].reshape(NH * QB, HEAD)
            nk = ss * CH + (qb + 1) * QB
            sbuf[qb % 2, :, pl.ds(0, nk)] = lax.dot_general(q4, kbuf[pl.ds(0, nk)], (((1,), (1,)), ((), ())), preferred_element_type=F32)

        def pref(qb, rows, cols):
            return prob.at[rows, cols] if qb % 2 == 0 else ou.at[rows, pl.ds(OW + F - S + cols.start, cols.size)]

        def softmax(ss, qb):
            full = ss * CH + qb * QB
            nk = full + QB
            sl = qb % 2
            rid = lax.broadcasted_iota(jnp.int32, (16, QB), 0)
            cid = lax.broadcasted_iota(jnp.int32, (16, QB), 1)
            for r in range(QB // 16):
                tri = jnp.where(cid <= rid + r * 16, 0.0, -1e30)
                for h in range(NH):
                    rows = pl.ds(h * QB + r * 16, 16)
                    t = sbuf[sl, rows, pl.ds(0, nk)] * sscale + lbias[:, pl.ds(0, nk)]
                    d = t[:, full:] + tri
                    m = jnp.max(d, axis=1, keepdims=True)
                    if full:
                        t = t[:, :full]
                        m = jnp.maximum(m, jnp.max(t, axis=1, keepdims=True))
                        e = jnp.exp2(t - m)
                        ed = jnp.exp2(d - m)
                        inv = 1.0 / (jnp.sum(e, axis=1, keepdims=True) + jnp.sum(ed, axis=1, keepdims=True))
                        pref(qb, rows, pl.ds(0, full))[...] = (e * inv).astype(BF)
                    else:
                        ed = jnp.exp2(d - m)
                        inv = 1.0 / jnp.sum(ed, axis=1, keepdims=True)
                    pref(qb, rows, pl.ds(full, QB))[...] = (ed * inv).astype(BF)

        def pv(ss, qb):
            nk = ss * CH + (qb + 1) * QB
            o = jnp.dot(pref(qb, pl.ds(0, CH), pl.ds(0, nk))[...], vbuf[pl.ds(0, nk)], preferred_element_type=F32).astype(BF)
            for h in range(NH):
                ou[pl.ds(qb * QB, QB), pl.ds(h * HEAD, HEAD)] = o[h * QB:(h + 1) * QB]

        lbias[...] = jnp.where(lax.broadcasted_iota(jnp.int32, lbias.shape, 1) < rlen, 0.0, -1e30)

        for ss in range(HS):
            @pl.when(s == ss)
            def _():
                qk(ss, 0)
                for qb in range(4):
                    if qb < 3:
                        qk(ss, qb + 1)
                    softmax(ss, qb)
                    pv(ss, qb)

        @pl.loop(2, NT)
        def _(j):
            wait(c_gu(i, j))

            @pl.when(j + 2 < NT)
            def _():
                start(c_gu(i, j + 2))

            @pl.when(j + 2 == NT)
            def _():
                start(c_dn(l, 0))

            @pl.when(j + 1 == NT)
            def _():
                start(c_dn(l, 1))

            @pl.when((j == 2) & more)
            def _():
                start(c_qkv(lnext))

            @pl.when(more)
            def _():
                c_hgu(i + 1, j - 2)[0].wait()

                @pl.when(j + 1 < NT)
                def _():
                    start_by_layer(i + 1, c_hgu(i + 1, j - 1))

                @pl.when(j + 1 == NT)
                def _():
                    start_by_layer(i + 1, c_hdn(i + 1, 0))
            for k, evs in GU_EV.items():
                events(i, evs, j == k)
            gu(j)
            ln_next(i, (j - 2) * UB, UB, lax.rem(j, 2))

        start_by_layer(i, c_res(i))

        @pl.loop(0, NG)
        def _(g):
            wait(c_dn(l, g))

            @pl.when((g >= 1) & (g + 1 < NG))
            def _():
                start(c_dn(l, g + 1))

            @pl.when((g >= 2) & more)
            def _():
                start(c_gu(i + 1, g - 2))

            @pl.when(more)
            def _():
                c_hdn(i + 1, g)[0].wait()

                @pl.when(g + 1 < NG)
                def _():
                    start_by_layer(i + 1, c_hdn(i + 1, g + 1))
            for k, evs in DN_EV.items():
                events(i, evs, g == k)
            pbuf[g] = jnp.dot(ou[...], wdn[lax.rem(g, 2)], preferred_element_type=F32).astype(BF)
            ln_next(i, UN * UB + g * US, US, lax.rem(UN + g, 2))
            k_d2d(i, g).start()
        events(i, END_EV)

    for name, lag, g in TAIL_EV:
        handlers[name](NC - lag, g)
    a0(NC - 2, 0)
    a0(NC - 1, 0)
    wait(c_kv(NC - 1))


def build(cfg, lens, x, cos, sin, wq, wk, wv, wo, wg, wu, wd, ng, qg, kg):
    CH, D, F, NH, HS = cfg["CH"], cfg["D"], cfg["F"], cfg["NH"], cfg["HS"]
    L, S = wq.shape[0], x.shape[1]
    OW = NH * HEAD
    GC = D // NG
    FT = cfg["FT"]
    any_ = pl.BlockSpec(memory_space=pltpu.HBM)
    vm = pl.BlockSpec(memory_space=pltpu.VMEM)
    V = pltpu.VMEM
    dma = pltpu.SemaphoreType.DMA
    T = 2 * S
    fl = L * (2 * T * D * (OW + 2 * HEAD + 2 * F) + 2 * T * (OW + F) * D)
    return pl.pallas_call(
        functools.partial(mega, cfg),
        name="mega",
        out_shape=(jax.ShapeDtypeStruct((L, 2, S, D), BF), jax.ShapeDtypeStruct((L, 2, S, HEAD), BF), jax.ShapeDtypeStruct((L, 2, S, HEAD), BF)),
        in_specs=[pl.BlockSpec(memory_space=pltpu.SMEM)] + [any_] * 10 + [vm] * 3,
        out_specs=(any_, any_, any_),
        scratch_shapes=[
            V((D, OW + 2 * HEAD), BF), V((3, D, 2 * FT), BF), V((2, OW + F, GC), BF),
            V((2, CH, D), BF), V((2, CH // 8, D), BF), V((CH, OW + F), BF),
            V((NG, CH, GC), BF), V((2, NG, CH // 2, GC), BF), V((2, NG, CH // 4, GC), BF), V((2, NG, CH // 8, GC), BF),
            V((CH // 8, D), BF), V((NH, CH, HEAD), BF), V((2, NH * CH // 4, S), F32), V((NH * CH // 4, S), BF), V((16, S), F32), V((S, HEAD), BF), V((S, HEAD), BF),
            V((2, CH, HEAD), F32),
            dma((KINDS, 2, NG)), dma((KINDS, 2, NG)), dma((6, 3)), dma((4, NG)), dma((2,)),
        ],
        compiler_params=pltpu.CompilerParams(collective_id=0, has_side_effects=True, vmem_limit_bytes=67 * 10 ** 6),
        cost_estimate=pl.CostEstimate(flops=fl, bytes_accessed=200 * 2 ** 20, transcendentals=0),
    )(lens, x, cos, sin, wq, wk, wv, wo, wg, wu, wd, ng, qg, kg)


def copy_out(hy, kc, vc, y, ko, vo, buf, kbuf, vbuf, sem, ksem):
    L = hy.shape[0]
    n = buf.shape[0]
    per = n // 2
    rows = hy.shape[2] // per
    cin, cout = [], []
    for k in range(n):
        at = (k // per, pl.ds(k % per * rows, rows))
        cin.append(pltpu.make_async_copy(hy.at[(L - 1,) + at], buf.at[k], sem.at[0, k]))
        cout.append(pltpu.make_async_copy(buf.at[k], y.at[at], sem.at[1, k]))
    for q, (src, tmp, dst) in enumerate(((kc, kbuf, ko), (vc, vbuf, vo))):
        cin.append(pltpu.make_async_copy(src, tmp, ksem.at[0, q]))
        cout.append(pltpu.make_async_copy(tmp, dst, ksem.at[1, q]))
    for cp in cin:
        cp.start()
    for a, b in zip(cin, cout):
        a.wait()
        b.start()
    for cp in cout:
        cp.wait()


def detach(hy, kc, vc):
    any_ = pl.BlockSpec(memory_space=pltpu.HBM)
    _, B, S, D = hy.shape
    n = 16
    return pl.pallas_call(
        copy_out, name="copy_out",
        out_shape=(jax.ShapeDtypeStruct((B, S, D), BF), jax.ShapeDtypeStruct(kc.shape, BF), jax.ShapeDtypeStruct(vc.shape, BF)),
        in_specs=[any_] * 3, out_specs=(any_,) * 3,
        scratch_shapes=[pltpu.VMEM((n, B * S // n, D), BF), pltpu.VMEM(kc.shape, BF), pltpu.VMEM(vc.shape, BF),
                        pltpu.SemaphoreType.DMA((2, n)), pltpu.SemaphoreType.DMA((2, 2))],
        compiler_params=pltpu.CompilerParams(vmem_limit_bytes=48 * 2 ** 20),
    )(hy, kc, vc)


def rope_tables(positions):
    pair = jnp.arange(HEAD // 2, dtype=F32) * (2.0 / HEAD)
    freq = jnp.repeat(ROPE_THETA ** (-pair), 2)
    ang = positions.astype(F32)[:, :, None] * freq
    sign = jnp.where(jnp.arange(HEAD) % 2 == 0, -1.0, 1.0).astype(F32)
    return jnp.cos(ang), jnp.sin(ang) * sign


def solution(mesh, ch=512, ft=256):
    act = P("dp", None, None)
    col = P(None, None, "tp")
    row = P(None, "tp", None)
    cache = P(None, "dp", None, "tp", None)

    def body(x, positions, lengths, w_q, w_k, w_v, w_o, w_gate, w_up, w_down, norm_gain, q_gain, k_gain):
        L, S = w_q.shape[0], x.shape[1]
        hs = S // ch
        cfg = dict(CH=ch, D=x.shape[2], F=w_gate.shape[2], NH=q_gain.shape[1], NC=L * 2 * hs, HS=hs, FT=ft)
        cos, sin = rope_tables(positions)
        hy, kc, vc = build(cfg, lengths, x, cos, sin, w_q, w_k, w_v, w_o, w_gate, w_up, w_down, norm_gain, q_gain, k_gain)
        y, kc, vc = detach(hy, kc, vc)
        return y, kc[:, :, :, None, :], vc[:, :, :, None, :]

    return jax.shard_map(body, mesh=mesh, in_specs=(act, P("dp", None), P("dp"), col, col, col, row, col, col, row, P(None, None), row, row),
                         out_specs=(act, cache, cache), check_vma=False)
```

```python
import functools
import math

import jax
import jax.numpy as jnp
from jax import lax
from jax.experimental import pallas as pl
from jax.experimental.pallas import tpu as pltpu
from jax.sharding import PartitionSpec as P

HEAD = 128
ROPE_THETA = 75000000.0
NORM_EPS = 1e-5
BF = jnp.bfloat16
F32 = jnp.float32
MESH = pl.DeviceIdType.MESH
NG = 4
KINDS = 9
D2D, S1, S2, A2, A1A, A1B, A0A, A0B, A0C = range(KINDS)

Q_EV = [("a1", 2, 2)]
ROPE_EV = {0: [("s0", 1, 3), ("s1", 1, 0), ("a1", 2, 3)], 1: [("s1", 1, 1)]}
ATT_EV = [("s1", 1, 2)]
GU_EV = {2: [("s2", 1, 0)], 3: [("s1", 1, 3), ("s2", 1, 1)], 4: [("s2", 1, 2), ("a0", 2, 0)], 5: [("s2", 1, 3), ("a2", 1, 0)], 6: [("a2", 1, 1)]}
DN_EV = {0: [("a2", 1, 2)], 1: [("a2", 1, 3), ("a1", 1, 0)], 2: [("s0", 0, 0)], 3: [("s0", 0, 1), ("a1", 1, 1)]}
END_EV = [("s0", 0, 2)]
TAIL_EV = [("a1", 2, 2), ("a1", 2, 3), ("s0", 1, 3), ("s1", 1, 0), ("s1", 1, 1), ("s2", 1, 0), ("s1", 1, 2), ("s2", 1, 1), ("a2", 1, 0), ("s1", 1, 3), ("s2", 1, 2), ("a2", 1, 1), ("a1", 1, 0),
           ("s2", 1, 3), ("a2", 1, 2), ("a1", 1, 1), ("a2", 1, 3), ("a1", 1, 2), ("a1", 1, 3)]


def mo(v, m):
    return pl.multiple_of(v, m)


def mega(cfg, lens, x, cos, sin, wq, wk, wv, wo, wg, wu, wd, ng, qg, kg,
         hy, kc, vc,
         wqkv, ring, wdn, nbuf, hblk, ou, pbuf, d2d, s1b, s2b, res, qbuf, sbuf, prob, lbias, kbuf, vbuf, csb,
         ssem, rsem, wsem, lsem, osem):
    CH, D, F, NH, NC, HS = cfg["CH"], cfg["D"], cfg["F"], cfg["NH"], cfg["NC"], cfg["HS"]
    GC = D // NG
    FT = cfg["FT"]
    NT = F // FT
    OW = NH * HEAD
    S = HS * CH
    QB = CH // 4
    tp = lax.axis_index("tp")
    core = lax.rem(tp, 2)
    bx = lax.rem(lax.div(tp, 2), 2)
    by = lax.div(tp, 4)
    xn = tp + 2 - 4 * bx
    yn = tp + 4 - 8 * by
    cn = tp + 1 - 2 * core
    n1 = jnp.where(core == 0, xn, yn)
    n2 = jnp.where(core == 0, yn, xn)
    b1 = jnp.where(core == 0, bx, by)
    b2 = jnp.where(core == 0, by, bx)
    H2, H4, H8 = CH // 2, CH // 4, CH // 8
    my_row = core * H2 + b1 * H4 + b2 * H8

    def where(c):
        l = lax.div(c, 2 * HS)
        b = lax.rem(lax.div(c, HS), 2)
        s = lax.rem(c, HS)
        return l, b, s

    def rcopy(kind, c, g, src, dst, dev):
        par = lax.rem(c, 2)
        return pltpu.make_async_remote_copy(
            src_ref=src, dst_ref=dst, send_sem=ssem.at[kind, par, g], recv_sem=rsem.at[kind, par, g],
            device_id={"tp": dev}, device_id_type=MESH)

    def hrows(c, off, n, g):
        l, b, s = where(c)
        return hy.at[l, b, pl.ds(mo(s * CH + off, H8), n), pl.ds(mo(g * GC, GC), GC)]

    def k_d2d(c, g):
        par = lax.rem(c, 2)
        return rcopy(D2D, c, g, pbuf.at[g, pl.ds(mo((1 - core) * H2, H2), H2)], d2d.at[par, g], cn)

    def k_s1(c, g):
        par = lax.rem(c, 2)
        return rcopy(S1, c, g, d2d.at[par, g, pl.ds(mo((1 - b1) * H4, H4), H4)], s1b.at[par, g], n1)

    def k_s2(c, g):
        par = lax.rem(c, 2)
        return rcopy(S2, c, g, s1b.at[par, g, pl.ds(mo((1 - b2) * H8, H8), H8)], s2b.at[par, g], n2)

    def k_own(kind, c, g, dev):
        return rcopy(kind, c, g, s2b.at[lax.rem(c, 2), g], hrows(c, my_row, H8, g), dev)

    def k_fwd(kind, c, g, dev):
        if kind == A0C:
            off, n = core * H2 + (1 - b1) * H4, H4
        else:
            off, n = core * H2 + b1 * H4 + (1 - b2) * H8, H8
        ref = hrows(c, off, n, g)
        return rcopy(kind, c, g, ref, ref, dev)

    def k_loc(c, g):
        return pltpu.make_async_copy(s2b.at[lax.rem(c, 2), g], hrows(c, my_row, H8, g), lsem.at[2 + lax.rem(c, 2), g])

    def c_res(c):
        l, b, s = where(c)
        rows = pl.ds(mo(s * CH + my_row, H8), H8)
        return (pltpu.make_async_copy(x.at[b, rows], res, lsem.at[1, 0]),
                pltpu.make_async_copy(hy.at[0, b, rows], res, lsem.at[1, 0]))

    RB = min(32, H8)

    def s0(c, g):
        par = lax.rem(c, 2)
        cp = k_d2d(c, g)
        cp.wait_recv()
        cp.wait_send()

        @pl.loop(0, H2 // RB)
        def _(r):
            rr = pl.ds(mo(r * RB, RB), RB)
            d2d[par, g, rr] = d2d[par, g, rr] + pbuf[g, pl.ds(mo(core * H2 + r * RB, RB), RB)]
        k_s1(c, g).start()

    def s1(c, g):
        par = lax.rem(c, 2)
        cp = k_s1(c, g)
        cp.wait_recv()
        cp.wait_send()

        @pl.loop(0, H4 // RB)
        def _(r):
            rr = pl.ds(mo(r * RB, RB), RB)
            s1b[par, g, rr] = s1b[par, g, rr] + d2d[par, g, pl.ds(mo(b1 * H4 + r * RB, RB), RB)]
        k_s2(c, g).start()

    def s2(c, g):
        par = lax.rem(c, 2)
        cp = k_s2(c, g)
        cp.wait_recv()
        cp.wait_send()
        if g == 0:
            c_res(c)[0].wait()

        @pl.loop(0, H8 // RB)
        def _(r):
            rr = pl.ds(mo(r * RB, RB), RB)
            t = s2b[par, g, rr].astype(F32) + s1b[par, g, pl.ds(mo(b2 * H8 + r * RB, RB), RB)].astype(F32)
            s2b[par, g, rr] = (t + res[rr, pl.ds(g * GC, GC)].astype(F32)).astype(BF)
        k_own(A2, c, g, n2).start()
        k_own(A1A, c, g, n1).start()
        k_own(A0A, c, g, cn).start()
        k_loc(c, g).start()

    def a2(c, g):
        cp = k_own(A2, c, g, n2)
        cp.wait_recv()
        cp.wait_send()
        k_fwd(A1B, c, g, n1).start()
        k_fwd(A0B, c, g, cn).start()

    def a1(c, g):
        for cp in (k_own(A1A, c, g, n1), k_fwd(A1B, c, g, n1)):
            cp.wait_recv()
            cp.wait_send()
        k_fwd(A0C, c, g, cn).start()

    def a0(c, _):
        for g in range(NG):
            for cp in (k_own(A0A, c, g, cn), k_fwd(A0B, c, g, cn), k_fwd(A0C, c, g, cn)):
                cp.wait_recv()
                cp.wait_send()
            k_loc(c, g).wait()

    handlers = {"s0": s0, "s1": s1, "s2": s2, "a2": a2, "a1": a1, "a0": a0}

    def events(i, evs, extra=None):
        for lag in (2, 1, 0):
            now = [(name, g) for name, d, g in evs if d == lag]
            if not now:
                continue
            ok = i >= lag

            @pl.when(ok if extra is None else ok & extra)
            def _():
                for name, g in now:
                    handlers[name](i - lag, g)

    def c_qkv(l):
        return (pltpu.make_async_copy(wq.at[l], wqkv.at[:, pl.ds(0, OW)], wsem.at[5, 0]),
                pltpu.make_async_copy(wk.at[l], wqkv.at[:, pl.ds(OW, HEAD)], wsem.at[5, 1]),
                pltpu.make_async_copy(wv.at[l], wqkv.at[:, pl.ds(OW + HEAD, HEAD)], wsem.at[5, 2]))

    def c_gu(c, j):
        l = where(c)[0]
        sl = lax.rem(c * NT + j, 3)
        cc = pl.ds(mo(j * FT, FT), FT)
        return (pltpu.make_async_copy(wg.at[l, :, cc], ring.at[sl, :, pl.ds(0, FT)], wsem.at[0, sl]),
                pltpu.make_async_copy(wu.at[l, :, cc], ring.at[sl, :, pl.ds(FT, FT)], wsem.at[1, sl]))

    def c_dn(l, g):
        sl = lax.rem(g, 2)
        cc = pl.ds(mo(g * GC, GC), GC)
        return (pltpu.make_async_copy(wo.at[l, :, cc], wdn.at[sl, pl.ds(0, OW)], wsem.at[2, sl]),
                pltpu.make_async_copy(wd.at[l, :, cc], wdn.at[sl, pl.ds(OW, F)], wsem.at[3, sl]))

    UB, UN = CH // 8, 5
    US = (CH - UN * UB) // NG

    def c_h(c, off, n, sl):
        l, b, s = where(c)
        rows = pl.ds(mo(s * CH + off, 16), n)
        dst = hblk.at[sl, pl.ds(0, n)]
        return (pltpu.make_async_copy(x.at[b, rows], dst, lsem.at[0, sl]),
                pltpu.make_async_copy(hy.at[0, b, rows], dst, lsem.at[0, sl]))

    def c_hgu(c, u):
        return c_h(c, u * UB, UB, lax.rem(u, 2))

    def c_hdn(c, g):
        return c_h(c, UN * UB + g * US, US, lax.rem(UN + g, 2))

    def c_cs(c):
        l, b, s = where(c)
        rows = pl.ds(mo(s * CH, CH), CH)
        return (pltpu.make_async_copy(cos.at[b, rows], csb.at[0], wsem.at[4, 0]),
                pltpu.make_async_copy(sin.at[b, rows], csb.at[1], wsem.at[4, 1]))

    def c_kv(c):
        l, b, s = where(c)
        rows = pl.ds(mo(s * CH, CH), CH)
        return (pltpu.make_async_copy(kbuf.at[rows], kc.at[l, b, rows], osem.at[0]),
                pltpu.make_async_copy(vbuf.at[rows], vc.at[l, b, rows], osem.at[1]))

    def start(cps):
        for cp in cps:
            cp.start(priority=1)

    def wait(cps):
        for cp in cps:
            cp.wait()

    def start_by_layer(c, pair):
        @pl.when(c < 2 * HS)
        def _():
            pair[0].start()

        @pl.when(c >= 2 * HS)
        def _():
            pair[1].start()

    bar = pltpu.get_barrier_semaphore()
    for dev in (xn, yn, cn):
        pl.semaphore_signal(bar, inc=1, device_id={"tp": dev}, device_id_type=MESH)

    def ln_rows(src, dst, gain, n):
        for q in range(n // 16):
            v = src(q).astype(F32)
            mean = jnp.sum(v, axis=1, keepdims=True) * (1.0 / D)
            v = v - mean
            var = jnp.sum(v * v, axis=1, keepdims=True) * (1.0 / D)
            dst(q, (v * lax.rsqrt(var + NORM_EPS) * gain).astype(BF))

    def ln_first(src, dst, gain, n):
        means = [jnp.sum(src(q).astype(F32), axis=1, keepdims=True) * (1.0 / D) for q in range(n // 16)]
        rs = []
        for q in range(n // 16):
            v = src(q).astype(F32) - means[q]
            rs.append(lax.rsqrt(jnp.sum(v * v, axis=1, keepdims=True) * (1.0 / D) + NORM_EPS))
        for q in range(n // 16):
            dst(q, ((src(q).astype(F32) - means[q]) * rs[q] * gain).astype(BF))

    def ln_next(i, off, n, sl):
        par = lax.rem(i + 1, 2)
        gain = ng[pl.ds(jnp.minimum(lax.div(i + 1, 2 * HS), ng.shape[0] - 1), 1), :]

        def put(q, v):
            nbuf[par, pl.ds(mo(off + q * 16, 16), 16), :] = v
        ln_rows(lambda q: hblk[sl, pl.ds(q * 16, 16), :], put, gain, n)

    def first(k):
        rows = pl.ds(mo(k * UB, UB), UB)
        return pltpu.make_async_copy(x.at[0, rows], nbuf.at[1, rows], lsem.at[2 + lax.div(k, 4), lax.rem(k, 4)])

    for k in range(8):
        first(k).start()
    start(c_qkv(0))
    for cp in c_cs(0):
        cp.start()
    start(c_gu(0, 0))
    start(c_gu(0, 1))
    gain0 = ng[pl.ds(0, 1), :]

    @pl.loop(0, 8)
    def _(k):
        first(k).wait()

        def put(q, v):
            nbuf[0, pl.ds(mo(k * UB + q * 16, 16), 16), :] = v
        ln_first(lambda q: nbuf[1, pl.ds(mo(k * UB + q * 16, 16), 16), :], put, gain0, UB)

    pl.semaphore_wait(bar, 3)
    lane = lax.broadcasted_iota(jnp.int32, (CH // 2, HEAD), 1)
    even = lax.rem(lane, 2) == 0

    @pl.loop(0, NC)
    def _(i):
        l, b, s = where(i)
        np_ = lax.rem(i, 2)
        more = i + 1 < NC
        lnext = where(i + 1)[0]

        wait(c_qkv(l))
        events(i, Q_EV)

        @pl.when(i > 0)
        def _():
            wait(c_kv(i - 1))
        wait(c_cs(i))
        sbuf[1, :, pl.ds(0, OW + 2 * HEAD)] = jnp.dot(nbuf[np_], wqkv[...], preferred_element_type=F32)

        def gu(j):
            r = jnp.dot(nbuf[np_], ring[lax.rem(i * NT + j, 3)], preferred_element_type=F32)
            ou[:, pl.ds(mo(OW + j * FT, 128), FT)] = (jax.nn.silu(r[:, :FT]) * r[:, FT:]).astype(BF)

        @pl.loop(0, 2)
        def _(j):
            wait(c_gu(i, j))
            start(c_gu(i, j + 2))
            for k, evs in ROPE_EV.items():
                events(i, evs, j == k)
            rr = pl.ds(mo(j * H2, H2), H2)
            ct = csb[0, rr]
            st = csb[1, rr]

            def norm_rope(v, gvec):
                mean = jnp.sum(v, axis=1, keepdims=True) * (1.0 / HEAD)
                v = v - mean
                var = jnp.sum(v * v, axis=1, keepdims=True) * (1.0 / HEAD)
                v = v * lax.rsqrt(var + NORM_EPS) * gvec
                sw = jnp.where(even, pltpu.roll(v, HEAD - 1, 1), pltpu.roll(v, 1, 1))
                return (v * ct + sw * st).astype(BF)
            for h in range(NH):
                qbuf[h, rr] = norm_rope(sbuf[1, rr, pl.ds(h * HEAD, HEAD)], qg[l, pl.ds(h, 1), :])
            ks = pl.ds(mo(s * CH + j * H2, H2), H2)
            kbuf[ks] = norm_rope(sbuf[1, rr, pl.ds(OW, HEAD)], kg[l])
            vbuf[ks] = sbuf[1, rr, pl.ds(OW + HEAD, HEAD)].astype(BF)
            gu(j)

        for cp in c_kv(i):
            cp.start()

        @pl.when(more)
        def _():
            for cp in c_cs(i + 1):
                cp.start()
            start_by_layer(i + 1, c_hgu(i + 1, 0))
        events(i, ATT_EV)
        rlen = lens[b]
        sscale = HEAD ** -0.5 * math.log2(math.e)

        def qk(ss, qb):
            q4 = qbuf[:, pl.ds(qb * QB, QB), :].reshape(NH * QB, HEAD)
            nk = ss * CH + (qb + 1) * QB
            sbuf[qb % 2, :, pl.ds(0, nk)] = lax.dot_general(q4, kbuf[pl.ds(0, nk)], (((1,), (1,)), ((), ())), preferred_element_type=F32)

        def pref(qb, rows, cols):
            return prob.at[rows, cols] if qb % 2 == 0 else ou.at[rows, pl.ds(OW + F - S + cols.start, cols.size)]

        def softmax(ss, qb):
            full = ss * CH + qb * QB
            nk = full + QB
            sl = qb % 2
            rid = lax.broadcasted_iota(jnp.int32, (16, QB), 0)
            cid = lax.broadcasted_iota(jnp.int32, (16, QB), 1)
            for r in range(QB // 16):
                tri = jnp.where(cid <= rid + r * 16, 0.0, -1e30)
                for h in range(NH):
                    rows = pl.ds(h * QB + r * 16, 16)
                    t = sbuf[sl, rows, pl.ds(0, nk)] * sscale + lbias[:, pl.ds(0, nk)]
                    d = t[:, full:] + tri
                    m = jnp.max(d, axis=1, keepdims=True)
                    if full:
                        t = t[:, :full]
                        m = jnp.maximum(m, jnp.max(t, axis=1, keepdims=True))
                        e = jnp.exp2(t - m)
                        ed = jnp.exp2(d - m)
                        inv = 1.0 / (jnp.sum(e, axis=1, keepdims=True) + jnp.sum(ed, axis=1, keepdims=True))
                        pref(qb, rows, pl.ds(0, full))[...] = (e * inv).astype(BF)
                    else:
                        ed = jnp.exp2(d - m)
                        inv = 1.0 / jnp.sum(ed, axis=1, keepdims=True)
                    pref(qb, rows, pl.ds(full, QB))[...] = (ed * inv).astype(BF)

        def pv(ss, qb):
            nk = ss * CH + (qb + 1) * QB
            o = jnp.dot(pref(qb, pl.ds(0, CH), pl.ds(0, nk))[...], vbuf[pl.ds(0, nk)], preferred_element_type=F32).astype(BF)
            for h in range(NH):
                ou[pl.ds(qb * QB, QB), pl.ds(h * HEAD, HEAD)] = o[h * QB:(h + 1) * QB]

        lbias[...] = jnp.where(lax.broadcasted_iota(jnp.int32, lbias.shape, 1) < rlen, 0.0, -1e30)

        for ss in range(HS):
            @pl.when(s == ss)
            def _():
                qk(ss, 0)
                for qb in range(4):
                    if qb < 3:
                        qk(ss, qb + 1)
                    softmax(ss, qb)
                    pv(ss, qb)

        @pl.loop(2, NT)
        def _(j):
            wait(c_gu(i, j))

            @pl.when(j + 2 < NT)
            def _():
                start(c_gu(i, j + 2))

            @pl.when(j + 2 == NT)
            def _():
                start(c_dn(l, 0))

            @pl.when(j + 1 == NT)
            def _():
                start(c_dn(l, 1))

            @pl.when((j == 2) & more)
            def _():
                start(c_qkv(lnext))

            @pl.when(more)
            def _():
                c_hgu(i + 1, j - 2)[0].wait()

                @pl.when(j + 1 < NT)
                def _():
                    start_by_layer(i + 1, c_hgu(i + 1, j - 1))

                @pl.when(j + 1 == NT)
                def _():
                    start_by_layer(i + 1, c_hdn(i + 1, 0))
            for k, evs in GU_EV.items():
                events(i, evs, j == k)
            gu(j)
            ln_next(i, (j - 2) * UB, UB, lax.rem(j, 2))

        start_by_layer(i, c_res(i))

        @pl.loop(0, NG)
        def _(g):
            wait(c_dn(l, g))

            @pl.when((g >= 1) & (g + 1 < NG))
            def _():
                start(c_dn(l, g + 1))

            @pl.when((g >= 2) & more)
            def _():
                start(c_gu(i + 1, g - 2))

            @pl.when(more)
            def _():
                c_hdn(i + 1, g)[0].wait()

                @pl.when(g + 1 < NG)
                def _():
                    start_by_layer(i + 1, c_hdn(i + 1, g + 1))
            for k, evs in DN_EV.items():
                events(i, evs, g == k)
            pbuf[g] = jnp.dot(ou[...], wdn[lax.rem(g, 2)], preferred_element_type=F32).astype(BF)
            ln_next(i, UN * UB + g * US, US, lax.rem(UN + g, 2))
            k_d2d(i, g).start()
        events(i, END_EV)

    for name, lag, g in TAIL_EV:
        handlers[name](NC - lag, g)
    a0(NC - 2, 0)
    a0(NC - 1, 0)
    wait(c_kv(NC - 1))


def build(cfg, lens, x, cos, sin, wq, wk, wv, wo, wg, wu, wd, ng, qg, kg):
    CH, D, F, NH, HS = cfg["CH"], cfg["D"], cfg["F"], cfg["NH"], cfg["HS"]
    L, S = wq.shape[0], x.shape[1]
    OW = NH * HEAD
    GC = D // NG
    FT = cfg["FT"]
    any_ = pl.BlockSpec(memory_space=pltpu.HBM)
    vm = pl.BlockSpec(memory_space=pltpu.VMEM)
    V = pltpu.VMEM
    dma = pltpu.SemaphoreType.DMA
    T = 2 * S
    fl = L * (2 * T * D * (OW + 2 * HEAD + 2 * F) + 2 * T * (OW + F) * D)
    return pl.pallas_call(
        functools.partial(mega, cfg),
        name="mega",
        out_shape=(jax.ShapeDtypeStruct((L, 2, S, D), BF), jax.ShapeDtypeStruct((L, 2, S, HEAD), BF), jax.ShapeDtypeStruct((L, 2, S, HEAD), BF)),
        in_specs=[pl.BlockSpec(memory_space=pltpu.SMEM)] + [any_] * 10 + [vm] * 3,
        out_specs=(any_, any_, any_),
        scratch_shapes=[
            V((D, OW + 2 * HEAD), BF), V((3, D, 2 * FT), BF), V((2, OW + F, GC), BF),
            V((2, CH, D), BF), V((2, CH // 8, D), BF), V((CH, OW + F), BF),
            V((NG, CH, GC), BF), V((2, NG, CH // 2, GC), BF), V((2, NG, CH // 4, GC), BF), V((2, NG, CH // 8, GC), BF),
            V((CH // 8, D), BF), V((NH, CH, HEAD), BF), V((2, NH * CH // 4, S), F32), V((NH * CH // 4, S), BF), V((16, S), F32), V((S, HEAD), BF), V((S, HEAD), BF),
            V((2, CH, HEAD), F32),
            dma((KINDS, 2, NG)), dma((KINDS, 2, NG)), dma((6, 3)), dma((4, NG)), dma((2,)),
        ],
        compiler_params=pltpu.CompilerParams(collective_id=0, has_side_effects=True, vmem_limit_bytes=67 * 10 ** 6),
        cost_estimate=pl.CostEstimate(flops=fl, bytes_accessed=200 * 2 ** 20, transcendentals=0),
    )(lens, x, cos, sin, wq, wk, wv, wo, wg, wu, wd, ng, qg, kg)


def copy_out(hy, kc, vc, y, ko, vo, buf, kbuf, vbuf, sem, ksem):
    L = hy.shape[0]
    n = buf.shape[0]
    per = n // 2
    rows = hy.shape[2] // per
    cin, cout = [], []
    for k in range(n):
        at = (k // per, pl.ds(k % per * rows, rows))
        cin.append(pltpu.make_async_copy(hy.at[(L - 1,) + at], buf.at[k], sem.at[0, k]))
        cout.append(pltpu.make_async_copy(buf.at[k], y.at[at], sem.at[1, k]))
    for q, (src, tmp, dst) in enumerate(((kc, kbuf, ko), (vc, vbuf, vo))):
        cin.append(pltpu.make_async_copy(src, tmp, ksem.at[0, q]))
        cout.append(pltpu.make_async_copy(tmp, dst, ksem.at[1, q]))
    for cp in cin:
        cp.start()
    for a, b in zip(cin, cout):
        a.wait()
        b.start()
    for cp in cout:
        cp.wait()


def detach(hy, kc, vc):
    any_ = pl.BlockSpec(memory_space=pltpu.HBM)
    _, B, S, D = hy.shape
    n = 16
    return pl.pallas_call(
        copy_out, name="copy_out",
        out_shape=(jax.ShapeDtypeStruct((B, S, D), BF), jax.ShapeDtypeStruct(kc.shape, BF), jax.ShapeDtypeStruct(vc.shape, BF)),
        in_specs=[any_] * 3, out_specs=(any_,) * 3,
        scratch_shapes=[pltpu.VMEM((n, B * S // n, D), BF), pltpu.VMEM(kc.shape, BF), pltpu.VMEM(vc.shape, BF),
                        pltpu.SemaphoreType.DMA((2, n)), pltpu.SemaphoreType.DMA((2, 2))],
        compiler_params=pltpu.CompilerParams(vmem_limit_bytes=48 * 2 ** 20),
    )(hy, kc, vc)


def rope_tables(positions):
    pair = jnp.arange(HEAD // 2, dtype=F32) * (2.0 / HEAD)
    freq = jnp.repeat(ROPE_THETA ** (-pair), 2)
    ang = positions.astype(F32)[:, :, None] * freq
    sign = jnp.where(jnp.arange(HEAD) % 2 == 0, -1.0, 1.0).astype(F32)
    return jnp.cos(ang), jnp.sin(ang) * sign


def solution(mesh, ch=512, ft=256):
    act = P("dp", None, None)
    col = P(None, None, "tp")
    row = P(None, "tp", None)
    cache = P(None, "dp", None, "tp", None)

    def body(x, positions, lengths, w_q, w_k, w_v, w_o, w_gate, w_up, w_down, norm_gain, q_gain, k_gain):
        L, S = w_q.shape[0], x.shape[1]
        hs = S // ch
        cfg = dict(CH=ch, D=x.shape[2], F=w_gate.shape[2], NH=q_gain.shape[1], NC=L * 2 * hs, HS=hs, FT=ft)
        cos, sin = rope_tables(positions)
        hy, kc, vc = build(cfg, lengths, x, cos, sin, w_q, w_k, w_v, w_o, w_gate, w_up, w_down, norm_gain, q_gain, k_gain)
        y, kc, vc = detach(hy, kc, vc)
        return y, kc[:, :, :, None, :], vc[:, :, :, None, :]

    return jax.shard_map(body, mesh=mesh, in_specs=(act, P("dp", None), P("dp"), col, col, col, row, col, col, row, P(None, None), row, row),
                         out_specs=(act, cache, cache), check_vma=False)
```
